32 devices in a mesh: up: 8 (over y, x, core), dn: 4 (over z).
Axes of the slice: x: 2, y: 2, z: 4, core: 2. Of those that a mesh axis runs over, the one named last changes fastest.
Arguments:
- start_vector: bfloat16 [13312, 13312], P('up', 'dn'), may hold values from -6 to 6
- hop_tiles: bfloat16 [104, 5, 128, 128], replicated, may hold values from -0.5 to 0.5
- tile_columns: int32 [104, 5], replicated, may hold values from 0 to 103, as said below
- tile_signs: int32 [104, 5], replicated, may hold values from 0 to 1
- occupation: int32 [16, 13312], replicated, may hold values from 0 to 1, as said below
Outputs:
- next_vector: bfloat16 [13312, 13312], P('up', 'dn')
- alphas: float32 [2], replicated
- betas: float32 [2], replicated
The draws below stay inside these ranges and needn't reach their ends.
Inputs may be any that keep to these rules, and one draw needn't show every extreme that they name: Each row of tile_columns names 5 different tile columns. Every column of occupation holds exactly 8 ones.
All inputs are finite; a program needn't handle non-finite values.
Results may differ from the reference program's by a relative error of at most 0.0065.
Values may be sent and summed in bfloat16 or wider, within the bound.
A program may use at most 256 MiB of HBM per device.

```python
import jax
import jax.numpy as jnp
from jax import lax

DETS = 13312
SITES = 16
TILE = 128
TILE_K = 5
STEPS = 2
TILES = 104


def draw_tile_columns(key, part):
    scores = jax.random.randint(key, (TILES, TILES), 0, 1 << 20) * TILES + jnp.arange(TILES, dtype=jnp.int32)[None, :]
    order = jnp.argsort(scores, axis=1)
    return order[:, :TILE_K].astype(jnp.int32)


def draw_occupation(key, part):
    scores = jax.random.randint(key, (DETS, SITES), 0, 1 << 20) * SITES + jnp.arange(SITES, dtype=jnp.int32)[None, :]
    ranks = jnp.argsort(jnp.argsort(scores, axis=1), axis=1)
    filled = (ranks < SITES // 2).astype(jnp.int32)
    return filled.T


def with_ends(drawn, key, smallest, high):
    dims = drawn.shape
    index_at = [jax.random.randint(jax.random.fold_in(key, axis), (), 0, dims[axis]) for axis in range(len(dims))]
    drawn = drawn.at[tuple(index_at)].set(smallest)
    longest = dims.index(max(dims))
    index_at[longest] = (index_at[longest] + 1) % dims[longest]
    return drawn.at[tuple(index_at)].set(high)


def block_scale(key, dims, shards, smallest, high):
    level = 1.0
    for dim, blocks in shards:
        draws = jax.random.uniform(jax.random.fold_in(jax.random.fold_in(key, 6), dim), (blocks,), jnp.float32, smallest / len(shards), high / len(shards))
        level = level * jnp.repeat(jnp.exp(draws), dims[dim] // blocks).reshape((-1,) + (1,) * (len(dims) - 1 - dim))
    return level


def bell_draw(rng, shape, spread, most, pieces=(), held_as=jnp.bfloat16):
    loudness = block_scale(rng, shape, pieces, -0.22, 0.18) if pieces else 1.0
    entries = jax.random.normal(rng, shape, jnp.float32) * spread * loudness
    return jnp.minimum(jnp.maximum(entries, -most), most).astype(held_as)


def setup_inputs(seed: int = 0) -> dict:
    seeds = jax.random.split(jax.random.key(seed), 6)
    start_vector = bell_draw(seeds[0], (DETS, DETS), 1.0, 6.0, ((0, 8), (1, 4)))
    hop_tiles = bell_draw(seeds[1], (TILES, TILE_K, TILE, TILE), TILE ** -0.5, 0.5)
    tile_columns = draw_tile_columns(jax.random.fold_in(seeds[5], 71), 0)
    tile_signs = with_ends(jax.random.randint(seeds[3], (TILES, TILE_K), 0, 2), jax.random.fold_in(seeds[3], 1), 0, 1).astype(jnp.int32)
    occupation = draw_occupation(jax.random.fold_in(seeds[5], 71), 0)
    return {"start_vector": start_vector, "hop_tiles": hop_tiles, "tile_columns": tile_columns, "tile_signs": tile_signs, "occupation": occupation}


coupling = 4.0

def hop_last(matrix, signed_wide, tile_columns):

    def one_block(part):
        cube = part.reshape(part.shape[0], TILES, TILE)
        picked = cube[:, tile_columns].astype(jnp.float32)
        result = jnp.einsum('ikab,mikb->mia', signed_wide, picked, precision=lax.Precision.HIGHEST)
        return result.reshape(part.shape)
    blocks = matrix.reshape(-1, 512, matrix.shape[1])
    return lax.map(one_block, blocks).reshape(matrix.shape)

def reference(start_vector, hop_tiles, tile_columns, tile_signs, occupation):
    signed = hop_tiles * (1 - 2 * tile_signs).astype(jnp.bfloat16)[:, :, None, None]
    signed_wide = signed.astype(jnp.float32)
    occupied = occupation.astype(jnp.bfloat16)
    diagonal = coupling * jnp.dot(occupied.T, occupied, preferred_element_type=jnp.float32)
    vector = start_vector.astype(jnp.float32)
    total = jnp.sum(vector * vector)
    vector = vector / jnp.maximum(jnp.sqrt(total), 1.0)
    previous = jnp.zeros_like(vector)
    beta_value = jnp.float32(0.0)
    alpha_list = []
    beta_list = []
    for iteration in range(STEPS):
        rounded = vector.astype(jnp.bfloat16)
        hopped_up = hop_last(rounded.T, signed_wide, tile_columns).T.astype(jnp.bfloat16)
        hopped_down = hop_last(rounded, signed_wide, tile_columns).astype(jnp.bfloat16)
        work = hopped_up.astype(jnp.float32) + hopped_down.astype(jnp.float32) + diagonal * vector - beta_value * previous
        intersect = jnp.sum(work * vector)
        work = work - intersect * vector
        residual = jnp.sum(work * work)
        beta_value = jnp.sqrt(jnp.maximum(residual, 1.0))
        previous = vector
        vector = work / beta_value
        alpha_list.append(intersect)
        beta_list.append(beta_value)
    return (vector.astype(jnp.bfloat16), jnp.stack(alpha_list), jnp.stack(beta_list))
```

```python
import functools

import jax
import jax.numpy as jnp
from jax import lax
from jax.experimental import pallas as pl
from jax.experimental.pallas import tpu as pltpu
from jax.sharding import PartitionSpec as P

STEPS = 2


coupling = 4.0


def hop_kernel(tile_k, tile, group, parts_tiles, columns_ref, x_ref, tiles_ref, out_ref):
    first = pl.program_id(0) * group

    def one_tile(t, carry):
        picked = []
        for k in range(tile_k):
            column = columns_ref[(first + t) * tile_k + k]
            at = pl.multiple_of(lax.rem(column, parts_tiles) * tile, tile)
            picked.append(x_ref[lax.div(column, parts_tiles), :, pl.ds(at, tile)])
        left = jnp.concatenate(picked, axis=1)
        result = jnp.dot(left, tiles_ref[t], preferred_element_type=jnp.float32)
        out_ref[0, :, pl.ds(pl.multiple_of(t * tile, tile), tile)] = result.astype(jnp.bfloat16)
        return carry

    lax.fori_loop(0, group, one_tile, 0)


def hop_blocks(x, stacked, columns, tile_k):
    parts, rows, width = x.shape
    tiles, depth, tile = stacked.shape
    if width % tile:
        joined = x.transpose(1, 0, 2).reshape(1, rows, parts * width)
        hopped = hop_blocks(joined, stacked, columns, tile_k)
        return hopped.reshape(rows, parts, width).transpose(1, 0, 2)
    parts_tiles = width // tile
    group = max(d for d in range(1, 17) if parts_tiles % d == 0)
    per_part = parts_tiles // group
    return pl.pallas_call(
        functools.partial(hop_kernel, tile_k, tile, group, parts_tiles),
        grid_spec=pltpu.PrefetchScalarGridSpec(
            num_scalar_prefetch=1,
            grid=(tiles // group,),
            in_specs=[
                pl.BlockSpec((parts, rows, width), lambda i, c: (0, 0, 0)),
                pl.BlockSpec((group, depth, tile), lambda i, c: (i, 0, 0)),
            ],
            out_specs=pl.BlockSpec(
                (1, rows, group * tile), lambda i, c: (i // per_part, 0, i % per_part)
            ),
        ),
        out_shape=jax.ShapeDtypeStruct(x.shape, jnp.bfloat16),
        compiler_params=pltpu.CompilerParams(vmem_limit_bytes=56 * 1024 * 1024),
        cost_estimate=pl.CostEstimate(
            flops=2 * rows * tiles * depth * tile,
            bytes_accessed=4 * rows * parts * width + 2 * tiles * depth * tile,
            transcendentals=0,
        ),
    )(columns, x, stacked)


def body(start_vector, hop_tiles, tile_columns, tile_signs, occupation):
    tiles, tile_k, tile, _ = hop_tiles.shape
    signed = hop_tiles * (1 - 2 * tile_signs).astype(jnp.bfloat16)[:, :, None, None]
    stacked = signed.transpose(0, 1, 3, 2).reshape(tiles, tile_k * tile, tile)
    columns = tile_columns.reshape(-1)
    block_rows, block_cols = start_vector.shape
    count_up = lax.axis_size("up")
    count_down = lax.axis_size("dn")
    row_start = lax.axis_index("up") * block_rows
    col_start = lax.axis_index("dn") * block_cols
    occ_rows = lax.dynamic_slice_in_dim(occupation, row_start, block_rows, 1).astype(jnp.bfloat16)
    occ_cols = lax.dynamic_slice_in_dim(occupation, col_start, block_cols, 1).astype(jnp.bfloat16)
    diagonal = (
        coupling * jnp.einsum("sa,sb->ab", occ_rows, occ_cols, preferred_element_type=jnp.float32)
    ).astype(jnp.bfloat16)
    total = lax.psum(jnp.sum(jnp.square(start_vector.astype(jnp.float32))), ("up", "dn"))
    scale = 1.0 / jnp.maximum(jnp.sqrt(total), 1.0)
    vector = start_vector.astype(jnp.float32) * scale
    length = total / jnp.maximum(total, 1.0)
    previous = None
    beta_value = None
    alpha_list = []
    beta_list = []
    for iteration in range(STEPS):
        rounded = start_vector if iteration == 0 else vector.astype(jnp.bfloat16)
        down = rounded.reshape(count_down, block_rows // count_down, block_cols)
        up = rounded.T.reshape(count_up, block_cols // count_up, block_rows)
        down = lax.all_to_all(down, "dn", 0, 0, tiled=True)
        up = lax.all_to_all(up, "up", 0, 0, tiled=True)
        down = hop_blocks(down, stacked, columns, tile_k)
        down = lax.all_to_all(down, "dn", 0, 0, tiled=True)
        up = hop_blocks(up, stacked, columns, tile_k)
        up = lax.all_to_all(up, "up", 0, 0, tiled=True)
        hopped_down = down.reshape(block_rows, block_cols)
        hopped_up = up.reshape(block_cols, block_rows).T
        hopped = hopped_up.astype(jnp.float32) + hopped_down.astype(jnp.float32)
        if iteration == 0:
            work = hopped * scale + diagonal * vector
        else:
            work = hopped + diagonal * vector - beta_value * previous
        intersect, square = lax.psum((jnp.sum(work * vector), jnp.sum(work * work)), ("up", "dn"))
        work = work - intersect * vector
        residual = square - 2.0 * intersect * intersect + intersect * intersect * length
        beta_value = jnp.sqrt(jnp.maximum(residual, 1.0))
        length = residual / jnp.maximum(residual, 1.0)
        previous = vector
        vector = work / beta_value
        alpha_list.append(intersect)
        beta_list.append(beta_value)
    final = vector.astype(jnp.bfloat16)
    return (final, jnp.stack(alpha_list), jnp.stack(beta_list))


def solution(mesh):
    placed = (P("up", "dn"), P(), P(), P(), P())
    return jax.shard_map(
        body, mesh=mesh, in_specs=placed, out_specs=(P("up", "dn"), P(), P()), check_vma=False
    )
```
